32 devices in a mesh: frame: 16 (over z, y, x), row: 2 (over core).
Axes of the slice: x: 2, y: 2, z: 4, core: 2. Of those that a mesh axis runs over, the one named last changes fastest.
Arguments:
- footage: float32 [64, 1024, 1024], P('frame', 'row'), may hold values from -30 to 30
Outputs:
- coefficients: float32 [64, 1024, 1024], P('frame', 'row')
- energies: float32 [4, 10], replicated
The draws below stay inside these ranges and needn't reach their ends.
All inputs are finite; a program needn't handle non-finite values.
Results may differ from the reference program's by a relative error of at most 0.00007.
Values sent between devices are 32-bit elements; how exact they have to be, the bound alone decides.
No kernel may reach another device: no remote copies, remote signals or barrier semaphores. Data moves between devices by JAX's collectives and lax.ppermute only.
A program may use at most 128 MiB of HBM per device.

```python
import math
from functools import partial
import jax
import jax.numpy as jnp
import numpy as np
from jax import lax

H = 1024
W = 1024
SLEVELS = 3
TLEVELS = 3
FRAMES = 64


def draw_footage(key, part):
    subkeys = jax.random.split(jax.random.fold_in(key, 7), 1)
    full_shape = (FRAMES, H, W)
    frame_ramp = jnp.arange(FRAMES, dtype=jnp.float32) / (FRAMES - 1)
    values = jnp.clip(jax.random.normal(subkeys[0], full_shape, jnp.float32), -5.0, 5.0)
    values = values * jnp.exp(math.log(3.0) * frame_ramp)[:, None, None]
    return values


def setup_inputs(seed: int = 0) -> dict:
    keys = jax.random.split(jax.random.key(seed), 2)
    return {
        "footage": draw_footage(jax.random.fold_in(keys[1], 71), 0),
    }


LIFT_ALPHA = -1.586134342
LIFT_BETA = -0.05298011854
LIFT_GAMMA = 0.8829110762
LIFT_DELTA = 0.4435068522
LIFT_ZETA = 1.149604398


def mirror_after(values, along):
    length = values.shape[along]
    return jnp.concatenate([lax.slice_in_dim(values, 1, length, axis=along), lax.slice_in_dim(values, length - 1, length, axis=along)], axis=along)


def mirror_before(values, along):
    length = values.shape[along]
    return jnp.concatenate([lax.slice_in_dim(values, 0, 1, axis=along), lax.slice_in_dim(values, 0, length - 1, axis=along)], axis=along)


def weave_axis(even_part, odd_part, along):
    stacked = jnp.stack([even_part, odd_part], axis=along + 1)
    new_shape = list(even_part.shape)
    new_shape[along] = new_shape[along] * 2
    return stacked.reshape(tuple(new_shape))


def lift_pair(even_part, odd_part, take_next, take_prev):
    odd_part = odd_part + LIFT_ALPHA * (even_part + take_next(even_part))
    even_part = even_part + LIFT_BETA * (take_prev(odd_part) + odd_part)
    odd_part = odd_part + LIFT_GAMMA * (even_part + take_next(even_part))
    even_part = even_part + LIFT_DELTA * (take_prev(odd_part) + odd_part)
    return even_part * LIFT_ZETA, odd_part * (1.0 / LIFT_ZETA)


def spatial(planes_in, levels, take_next, take_prev):
    row_axis = planes_in.ndim - 2
    col_axis = planes_in.ndim - 1
    low_cols, high_cols = lift_pair(planes_in[..., 0::2], planes_in[..., 1::2], partial(mirror_after, along=col_axis), partial(mirror_before, along=col_axis))
    combined = jnp.concatenate([low_cols, high_cols], axis=col_axis)
    low_rows, high_rows = lift_pair(combined[..., 0::2, :], combined[..., 1::2, :], take_next, take_prev)
    half_width = low_cols.shape[-1]
    coarse = low_rows[..., :half_width]
    if levels > 1:
        coarse = spatial(coarse, levels - 1, take_next, take_prev)
    upper_rows = weave_axis(coarse, low_rows[..., half_width:], col_axis)
    bottom = weave_axis(high_rows[..., :half_width], high_rows[..., half_width:], col_axis)
    return weave_axis(upper_rows, bottom, row_axis)


def temporal(planes_in, levels):
    even_part = planes_in[0::2]
    odd_part = planes_in[1::2]
    odd_part = odd_part - 0.5 * (even_part + mirror_after(even_part, 0))
    even_part = even_part + 0.25 * (mirror_before(odd_part, 0) + odd_part)
    if levels > 1:
        even_part = temporal(even_part, levels - 1)
    return weave_axis(even_part, odd_part, 0)


def level_of(number, ceiling):
    depth_now = 1
    while number % 2 == 0 and depth_now <= ceiling:
        number = number // 2
        depth_now = depth_now + 1
    return depth_now


def space_table(levels):
    period = 2 ** levels
    band_table = np.zeros((period * period, 3 * levels + 1), np.float32)
    for row_pos in range(period):
        for col_pos in range(period):
            row_level = level_of(row_pos, levels)
            col_level = level_of(col_pos, levels)
            finest = min(row_level, col_level)
            if finest > levels:
                column = 3 * levels
            elif row_level == col_level:
                column = 3 * (finest - 1) + 2
            elif row_level == finest:
                column = 3 * (finest - 1)
            else:
                column = 3 * (finest - 1) + 1
            band_table[row_pos * period + col_pos, column] = 1.0
    return band_table


def time_table(levels):
    period = 2 ** levels
    band_table = np.zeros((period, levels + 1), np.float32)
    for number in range(period):
        band_table[number, level_of(number, levels) - 1] = 1.0
    return band_table


def band_sums(coeffs, first_frame, levels_s, levels_t):
    period = 2 ** levels_s
    frame_count, row_count, col_count = coeffs.shape
    square = coeffs * coeffs
    pattern = square.reshape(frame_count, row_count // period, period, col_count // period, period).sum(axis=(1, 3))
    pattern = pattern.reshape(frame_count, period * period)
    per_frame = jnp.dot(pattern, jnp.asarray(space_table(levels_s), jnp.float32), precision=lax.Precision.HIGHEST)
    time_period = 2 ** levels_t
    position = (first_frame + jnp.arange(frame_count, dtype=jnp.int32)) % time_period
    onehot = (position[:, None] == jnp.arange(time_period, dtype=jnp.int32)[None, :]).astype(jnp.float32)
    frame_band = jnp.dot(onehot, jnp.asarray(time_table(levels_t), jnp.float32), precision=lax.Precision.HIGHEST)
    return jnp.dot(frame_band.T, per_frame, precision=lax.Precision.HIGHEST)


def band_means(totals, frames_all, rows_all, cols_all, levels_s, levels_t):
    space_share = space_table(levels_s).sum(0) / float((2 ** levels_s) ** 2)
    time_share = time_table(levels_t).sum(0) / float(2 ** levels_t)
    counts = float(frames_all) * float(rows_all) * float(cols_all) * np.outer(time_share, space_share)
    return totals / jnp.asarray(counts, jnp.float32)


def reference(footage):
    frames_all, rows_all, cols_all = footage.shape

    def picture_step(picture):
        return spatial(picture[None], SLEVELS, partial(mirror_after, along=1), partial(mirror_before, along=1))[0]

    planes = lax.map(picture_step, footage)
    block_rows = 8
    grouped = jnp.moveaxis(planes.reshape(frames_all, rows_all // block_rows, block_rows, cols_all), 1, 0)

    def time_step(row_block):
        return temporal(row_block, TLEVELS)

    temporal_out = lax.map(time_step, grouped)
    coeffs = jnp.moveaxis(temporal_out, 0, 1).reshape(frames_all, rows_all, cols_all)
    totals = band_sums(coeffs, 0, SLEVELS, TLEVELS)
    return coeffs, band_means(totals, frames_all, rows_all, cols_all, SLEVELS, TLEVELS)
```

```python
import functools

import jax
import jax.numpy as jnp
import numpy as np
from jax import lax
from jax.experimental import pallas as pl
from jax.experimental.pallas import tpu as pltpu
from jax.sharding import PartitionSpec as P


SLEVELS = 3
TLEVELS = 3

LIFT_ALPHA = -1.586134342
LIFT_BETA = -0.05298011854
LIFT_GAMMA = 0.8829110762
LIFT_DELTA = 0.4435068522
LIFT_ZETA = 1.149604398
FACTORS = (LIFT_ALPHA, LIFT_BETA, LIFT_GAMMA, LIFT_DELTA)

LANES = 128
SUB = 8
HALO = 32
PAD = SUB
CHUNKS = 2
SPAN = 2 * 2**TLEVELS
KEPT = (0, 2, 3)


def level_of(number, ceiling):
    depth_now = 1
    while number % 2 == 0 and depth_now <= ceiling:
        number = number // 2
        depth_now = depth_now + 1
    return depth_now


def space_table(levels):
    period = 2**levels
    band_table = np.zeros((period * period, 3 * levels + 1), np.float32)
    for row_pos in range(period):
        for col_pos in range(period):
            row_level = level_of(row_pos, levels)
            col_level = level_of(col_pos, levels)
            finest = min(row_level, col_level)
            if finest > levels:
                column = 3 * levels
            elif row_level == col_level:
                column = 3 * (finest - 1) + 2
            elif row_level == finest:
                column = 3 * (finest - 1)
            else:
                column = 3 * (finest - 1) + 1
            band_table[row_pos * period + col_pos, column] = 1.0
    return band_table


def time_table(levels):
    period = 2**levels
    band_table = np.zeros((period, levels + 1), np.float32)
    for number in range(period):
        band_table[number, level_of(number, levels) - 1] = 1.0
    return band_table


def band_means(totals, frames_all, rows_all, cols_all, levels_s, levels_t):
    space_share = space_table(levels_s).sum(0) / float((2**levels_s) ** 2)
    time_share = time_table(levels_t).sum(0) / float(2**levels_t)
    counts = (
        float(frames_all) * float(rows_all) * float(cols_all) * np.outer(time_share, space_share)
    )
    return totals / jnp.asarray(counts, jnp.float32)


def lift_rows(buf, count):
    groups = count // SUB

    def step(odd, factor):
        target, near, far = (1, 0, 2) if odd else (0, -1, 1)

        def body(k, carry):
            top = PAD + 2 * SUB * k
            at = pl.ds(top + target, SUB, stride=2)
            for j in range(buf.shape[0]):
                buf[j, at, :] = buf[j, at, :] + factor * (
                    buf[j, pl.ds(top + near, SUB, stride=2), :]
                    + buf[j, pl.ds(top + far, SUB, stride=2), :]
                )
            return carry

        lax.fori_loop(0, groups, body, 0, unroll=2)

    step(True, LIFT_ALPHA)
    step(False, LIFT_BETA)
    step(True, LIFT_GAMMA)
    step(False, LIFT_DELTA)


def filter_taps():
    size = 8 * len(FACTORS)
    lifted = np.eye(size)
    for count, factor in enumerate(FACTORS):
        for n in range(1 - count % 2, size - 1, 2):
            lifted[n] += factor * (lifted[n - 1] + lifted[n + 1])
    middle = size // 2
    reach = len(FACTORS) + 1
    low = [lifted[middle, middle + k] * LIFT_ZETA for k in range(reach)]
    high = [lifted[middle + 1, middle + 1 + k] / LIFT_ZETA for k in range(reach)]
    return low, high


def lift_cols(buf, first, rows, stride):
    blocks = buf.shape[0]
    lane = lax.broadcasted_iota(jnp.int32, (SUB, LANES), 1)
    sub = lax.broadcasted_iota(jnp.int32, (SUB, LANES), 0)
    phase = lane % (2 * stride)
    low, high = filter_taps()
    reach = len(low)
    row_scale = jnp.where(sub % 2 == 0, jnp.float32(LIFT_ZETA), jnp.float32(1.0 / LIFT_ZETA))
    taps = [
        row_scale
        * jnp.where(
            phase == 0, jnp.float32(low[k]), jnp.where(phase == stride, jnp.float32(high[k]), 0.0)
        )
        for k in range(reach)
    ]
    shifts = [k * stride for k in range(reach)]
    head = [lane < shift for shift in shifts]
    tail = [lane >= LANES - shift for shift in shifts]

    def mirrored(x, source):
        return jnp.take_along_axis(x, source % LANES, axis=1)

    def body(i, carry):
        at = pl.ds(first + SUB * i, SUB)
        v = [buf[j, at, :] for j in range(blocks)]
        sums = [taps[0] * x for x in v]
        for k in range(1, reach):
            shift = shifts[k]
            up = [pltpu.roll(x, shift, 1) for x in v]
            down = [pltpu.roll(x, LANES - shift, 1) for x in v]
            left = mirrored(v[0], shift - lane)
            right = mirrored(v[-1], 2 * LANES - 2 * stride - shift - lane)
            for j in range(blocks):
                before = jnp.where(head[k], left if j == 0 else up[j - 1], up[j])
                after = jnp.where(tail[k], right if j == blocks - 1 else down[j + 1], down[j])
                sums[j] = sums[j] + taps[k] * (before + after)
        for j in range(blocks):
            buf[j, at, :] = sums[j]
        return carry

    lax.fori_loop(0, rows // SUB, body, 0, unroll=6)


def spatial_frame(x_ref, top_ref, bottom_ref, bufs):
    rows, width = x_ref.shape
    row_index = lax.axis_index("row")
    is_first = row_index == 0
    is_last = row_index == lax.axis_size("row") - 1
    first = PAD + HALO
    end = first + rows
    b = bufs[0]
    for j in range(width // LANES):
        c = slice(j * LANES, (j + 1) * LANES)
        b[j, first:end, :] = x_ref[:, c]
        b[j, PAD:first, :] = top_ref[:, c]
        b[j, end : end + HALO, :] = bottom_ref[:, c]

    @pl.when(is_first)
    def _():
        for j in range(1, HALO):
            b[:, first - j : first - j + 1, :] = b[:, first + j : first + j + 1, :]

    total = rows + 2 * HALO
    for level in range(SLEVELS):
        b = bufs[level]
        stride = 2**level
        count = total // stride
        inner = HALO // stride
        stop = PAD + inner + rows // stride

        @pl.when(is_last)
        def _(b=b, stop=stop, level=level, inner=inner):
            for j in range(inner - 1 if level == 0 else inner * 5 // 8):
                b[:, stop + j : stop + j + 1, :] = b[:, stop - 2 - j : stop - 1 - j, :]

        lift_rows(b, count // 2)
        lift_cols(b, PAD, count, stride)
        if level + 1 < SLEVELS:
            low = bufs[level + 1]

            def body(k, carry, b=b, low=low):
                for j in range(b.shape[0]):
                    low[j, pl.ds(PAD + SUB * k, SUB), :] = b[
                        j, pl.ds(PAD + 2 * SUB * k, SUB, stride=2), :
                    ]
                return carry

            lax.fori_loop(0, count // 2 // SUB, body, 0)
    lane = lax.broadcasted_iota(jnp.int32, (SUB, LANES), 1)
    for level in reversed(range(SLEVELS - 1)):
        b, low = bufs[level], bufs[level + 1]
        stride = 2 ** (level + 1)
        keep = lane % stride == 0

        def body(k, carry, b=b, low=low, keep=keep, stride=stride):
            at = pl.ds(PAD + HALO // (stride // 2) + 2 * SUB * k, SUB, stride=2)
            inner = pl.ds(PAD + HALO // stride + SUB * k, SUB)
            for j in range(b.shape[0]):
                b[j, at, :] = jnp.where(keep, low[j, inner, :], b[j, at, :])
            return carry

        lax.fori_loop(0, rows // stride // SUB, body, 0)


def member(group):
    return lax.axis_index("frame") % group


def space_first_kernel(group, x_ref, top_ref, bottom_ref, *refs):
    pieces, plane, bufs = refs[:group], refs[group], refs[group + 1 :]
    spatial_frame(x_ref.at[0], top_ref.at[0], bottom_ref.at[0], bufs)
    rows = x_ref.shape[1]
    first = PAD + HALO
    me = member(group)
    part = rows // group
    for d in range(group):
        start = pl.multiple_of(first + (me ^ d) * part, SUB)
        for j in range(bufs[0].shape[0]):
            c = slice(j * LANES, (j + 1) * LANES)
            pieces[d][0, :, c] = bufs[0][j, pl.ds(start, part), :]
    for j in range(bufs[0].shape[0]):
        plane[:, j * LANES : (j + 1) * LANES] = bufs[0][j, first : first + rows, :]


def space_rest_kernel(group, x_ref, top_ref, bottom_ref, plane_ref, *refs):
    count = group * CHUNKS
    pieces, out, held, bufs = refs[:count], refs[count], refs[count + 1], refs[count + 2 :]
    spatial_frame(x_ref.at[0], top_ref.at[0], bottom_ref.at[0], bufs)
    rows = x_ref.shape[1]
    first = PAD + HALO
    me = member(group)
    part = rows // group
    piece = part // CHUNKS
    for d in range(group):
        for c in range(CHUNKS):
            start = pl.multiple_of(first + (me ^ d) * part + c * piece, SUB)
            for j in range(bufs[0].shape[0]):
                at = slice(j * LANES, (j + 1) * LANES)
                pieces[d * CHUNKS + c][0, :, at] = bufs[0][j, pl.ds(start, piece), :]

    @pl.when(pl.program_id(0) == 0)
    def _():
        for j in range(bufs[0].shape[0]):
            at = slice(j * LANES, (j + 1) * LANES)
            held[j] = bufs[0][j, first : first + rows, :] - 0.5 * plane_ref[:, at]

    @pl.when(pl.program_id(0) == 1)
    def _():
        for j in range(bufs[0].shape[0]):
            at = slice(j * LANES, (j + 1) * LANES)
            out[0, :, at] = held[j] - 0.5 * bufs[0][j, first : first + rows, :]


def space_scratch(rows, width):
    total = rows + 2 * HALO
    return [
        pltpu.VMEM((width // LANES, total // 2**level + 2 * PAD, LANES), jnp.float32)
        for level in range(SLEVELS)
    ]


def space(footage, top, bottom, group):
    frames, rows, width = footage.shape
    part = rows // group
    piece = part // CHUNKS
    f32 = jnp.float32

    def ins(shift):
        return [
            pl.BlockSpec((1, rows, width), lambda g: (g + shift, 0, 0)),
            pl.BlockSpec((1, HALO, width), lambda g: (g + shift, 0, 0)),
            pl.BlockSpec((1, HALO, width), lambda g: (g + shift, 0, 0)),
        ]

    def cost(count):
        return pl.CostEstimate(
            flops=count * rows * width * 400, bytes_accessed=count * rows * width * 8, transcendentals=0
        )

    outs = pl.pallas_call(
        functools.partial(space_first_kernel, group),
        grid=(1,),
        in_specs=ins(0),
        out_specs=[pl.BlockSpec((1, part, width), lambda g: (0, 0, 0))] * group
        + [pl.BlockSpec((rows, width), lambda g: (0, 0))],
        out_shape=[jax.ShapeDtypeStruct((1, part, width), f32)] * group
        + [jax.ShapeDtypeStruct((rows, width), f32)],
        scratch_shapes=space_scratch(rows, width),
        cost_estimate=cost(1),
        name="space_first",
    )(footage, top, bottom)
    firsts, plane = outs[:group], outs[group]
    outs = pl.pallas_call(
        functools.partial(space_rest_kernel, group),
        grid=(frames - 1,),
        in_specs=ins(1) + [pl.BlockSpec((rows, width), lambda g: (0, 0))],
        out_specs=[pl.BlockSpec((1, piece, width), lambda g: (g, 0, 0))] * (group * CHUNKS)
        + [pl.BlockSpec((1, rows, width), lambda g: (1, 0, 0))],
        out_shape=[jax.ShapeDtypeStruct((frames - 1, piece, width), f32)] * (group * CHUNKS)
        + [jax.ShapeDtypeStruct((frames, rows, width), f32)],
        scratch_shapes=[pltpu.VMEM((width // LANES, rows, LANES), f32)] + space_scratch(rows, width),
        cost_estimate=cost(frames - 1),
        name="space_rest",
    )(footage, top, bottom, plane)
    rest = [[outs[d * CHUNKS + c] for d in range(group)] for c in range(CHUNKS)]
    return firsts, rest, outs[-1]


WIDE = 2 * LANES
BLOCK_ROWS = 16


def gather_span(group, firsts, rest, span):
    me = member(group)
    for d in range(group):
        base = (me ^ d) * (SPAN // group)
        span[base] = firsts[d][0]
        for f in range(SPAN // group - 1):
            span[base + 1 + f] = rest[d][f]


def each_tile(rows, width, body):
    tiles = width // WIDE

    def step(k, carry):
        r = pl.multiple_of((k // tiles) * SUB, SUB)
        c = pl.multiple_of((k % tiles) * WIDE, WIDE)
        body(pl.ds(r, SUB), pl.ds(c, WIDE))
        return carry

    lax.fori_loop(0, rows // SUB * tiles, step, 0)


def partial_levels(x):
    o = {n: x[n] - 0.5 * (x[n - 1] + x[n + 1]) for n in range(1, SPAN - 1, 2)}
    o[15] = x[15] - 0.5 * x[14]
    low = {n: x[n] + 0.25 * (o[n - 1] + o[n + 1]) for n in range(2, SPAN, 2)}
    low[0] = x[0] + 0.25 * o[1]
    p = {n: low[n] - 0.5 * (low[n - 2] + low[n + 2]) for n in (2, 6, 10)}
    p[14] = low[14] - 0.5 * low[12]
    m = {n: low[n] + 0.25 * (p[n - 2] + p[n + 2]) for n in (8, 12)}
    m[0] = low[0] + 0.25 * p[2]
    q12 = m[12] - 0.5 * m[8]
    to_right = (o[15], p[14], q12)
    to_left = (x[0], low[0], m[0])
    return to_right, to_left


def full_levels(x, left, right, is_first, is_last):
    a0, b0, c0 = left
    x16, low16, m16 = right
    o = {n: x[n] - 0.5 * (x[n - 1] + x[n + 1]) for n in range(1, SPAN - 1, 2)}
    o[15] = x[15] - 0.5 * (x[14] + jnp.where(is_last, x[14], x16))
    before = jnp.where(is_first, o[1], a0 - 0.5 * x[0])
    low = {n: x[n] + 0.25 * (o[n - 1] + o[n + 1]) for n in range(2, SPAN, 2)}
    low[0] = x[0] + 0.25 * (before + o[1])
    p = {n: low[n] - 0.5 * (low[n - 2] + low[n + 2]) for n in (2, 6, 10)}
    p[14] = low[14] - 0.5 * (low[12] + jnp.where(is_last, low[12], low16 + 0.25 * o[15]))
    before = jnp.where(is_first, p[2], b0 - 0.125 * x[0] - 0.5 * low[0])
    m = {n: low[n] + 0.25 * (p[n - 2] + p[n + 2]) for n in (4, 8, 12)}
    m[0] = low[0] + 0.25 * (before + p[2])
    q4 = m[4] - 0.5 * (m[0] + m[8])
    after = jnp.where(is_last, m[8], m16 + 0.21875 * o[15] + 0.25 * p[14])
    q12 = m[12] - 0.5 * (m[8] + after)
    before = jnp.where(is_first, q4, c0 - 0.03125 * x[0] - 0.125 * low[0] - 0.5 * m[0])
    y = dict(o)
    y.update(p)
    y[4] = q4
    y[12] = q12
    y[0] = m[0] + 0.25 * (before + q4)
    y[8] = m[8] + 0.25 * (q4 + q12)
    return [y[n] for n in range(SPAN)]


def edges_kernel(group, *refs):
    firsts, rest = refs[:group], refs[group : 2 * group]
    to_right, to_left, span = refs[2 * group :]
    gather_span(group, firsts, rest, span)
    _, rows, width = span.shape

    def body(r, c):
        right, left = partial_levels([span[n, r, c] for n in range(SPAN)])
        for k in range(TLEVELS):
            to_right[k, r, c] = right[k]
            to_left[k, r, c] = left[k]

    each_tile(rows, width, body)


def time_kernel(group, *refs):
    firsts, rest = refs[:group], refs[group : 2 * group]
    left, right = refs[2 * group : 2 * group + 2]
    pieces = refs[2 * group + 2 : 3 * group + 2]
    power, span = refs[3 * group + 2 :]
    gather_span(group, firsts, rest, span)
    _, rows, width = span.shape
    spot = lax.axis_index("frame") // group
    is_first = spot == 0
    is_last = spot == lax.axis_size("frame") // group - 1

    @pl.when(pl.program_id(0) == 0)
    def _():
        power[...] = jnp.zeros_like(power)

    def body(r, c):
        y = full_levels(
            [span[n, r, c] for n in range(SPAN)],
            [left[k, r, c] for k in range(TLEVELS)],
            [right[k, r, c] for k in range(TLEVELS)],
            is_first,
            is_last,
        )
        sums = [None] * (TLEVELS + 1)
        for n in range(SPAN):
            t = level_of(n % 2**TLEVELS, TLEVELS) - 1
            square = y[n] * y[n]
            sums[t] = square if sums[t] is None else sums[t] + square
            span[n, r, c] = y[n]
        for t in range(TLEVELS + 1):
            power[t, :, c] = power[t, :, c] + sums[t]

    each_tile(rows, width, body)
    me = member(group)
    for d in range(group):
        base = (me ^ d) * (SPAN // group)
        for k, f in enumerate(KEPT):
            pieces[d][k] = span[base + f]


def span_specs(group, chunk, piece, width):
    steps = piece // BLOCK_ROWS
    return [
        pl.BlockSpec((1, BLOCK_ROWS, width), lambda i: (0, chunk * steps + i, 0))
    ] * group + [pl.BlockSpec((SPAN // group - 1, BLOCK_ROWS, width), lambda i: (0, i, 0))] * group


def span_cost(piece, width, flops, frames):
    return pl.CostEstimate(
        flops=piece * width * flops, bytes_accessed=piece * width * 4 * frames, transcendentals=0
    )


def edges(group, chunk, firsts, rest):
    _, piece, width = rest[0].shape
    spec = pl.BlockSpec((TLEVELS, BLOCK_ROWS, width), lambda i: (0, i, 0))
    shape = jax.ShapeDtypeStruct((TLEVELS, piece, width), jnp.float32)
    return pl.pallas_call(
        functools.partial(edges_kernel, group),
        grid=(piece // BLOCK_ROWS,),
        in_specs=span_specs(group, chunk, piece, width),
        out_specs=[spec, spec],
        out_shape=[shape, shape],
        scratch_shapes=[pltpu.VMEM((SPAN, BLOCK_ROWS, width), jnp.float32)],
        cost_estimate=span_cost(piece, width, 2000, SPAN + 6),
    )(*firsts, *rest)


def finish_time(group, chunk, firsts, rest, left, right):
    _, piece, width = rest[0].shape
    kept = len(KEPT)
    halo = pl.BlockSpec((TLEVELS, BLOCK_ROWS, width), lambda i: (0, i, 0))
    outs = pl.pallas_call(
        functools.partial(time_kernel, group),
        grid=(piece // BLOCK_ROWS,),
        in_specs=span_specs(group, chunk, piece, width) + [halo, halo],
        out_specs=[pl.BlockSpec((kept, BLOCK_ROWS, width), lambda i: (0, i, 0))] * group
        + [pl.BlockSpec((TLEVELS + 1, SUB, width), lambda i: (0, 0, 0))],
        out_shape=[jax.ShapeDtypeStruct((kept, piece, width), jnp.float32)] * group
        + [jax.ShapeDtypeStruct((TLEVELS + 1, SUB, width), jnp.float32)],
        scratch_shapes=[pltpu.VMEM((SPAN, BLOCK_ROWS, width), jnp.float32)],
        cost_estimate=span_cost(piece, width, 2000, 2 * SPAN + 6),
    )(*firsts, *rest, left, right)
    return outs[:group], outs[group]


def place_kernel(group, chunk, *refs):
    pieces, out, sems = refs[:group], refs[group + 1], refs[group + 2]
    k = pl.program_id(0)
    frame = jnp.where(k == 0, KEPT[0], k + 1)
    _, rows, _ = pieces[0].shape
    part = rows * CHUNKS
    me = member(group)
    copies = []
    for d in range(group):
        start = pl.multiple_of((me ^ d) * part + chunk * rows, SUB)
        copies.append(
            pltpu.make_async_copy(pieces[d].at[0], out.at[frame, pl.ds(start, rows)], sems.at[d])
        )
    for copy in copies:
        copy.start()
    for copy in copies:
        copy.wait()


def place(group, chunk, pieces, coeffs):
    kept, piece, width = pieces[0].shape
    return pl.pallas_call(
        functools.partial(place_kernel, group, chunk),
        grid=(kept,),
        in_specs=[pl.BlockSpec((1, piece, width), lambda k: (k, 0, 0))] * group
        + [pl.BlockSpec(memory_space=pl.ANY)],
        out_specs=pl.BlockSpec(memory_space=pl.ANY),
        out_shape=jax.ShapeDtypeStruct(coeffs.shape, coeffs.dtype),
        input_output_aliases={group: 0},
        scratch_shapes=[pltpu.SemaphoreType.DMA((group,))],
        cost_estimate=span_cost(piece, width, 100, 2 * kept * group),
    )(*pieces, coeffs)


def swap(blocks, group):
    devices = range(lax.axis_size("frame"))
    out = [blocks[0]]
    for d in range(1, group):
        out.append(lax.ppermute(blocks[d], "frame", [(i, i ^ d) for i in devices]))
    return out


def shifted(block, axis, distance):
    devices = range(lax.axis_size(axis))
    route = [(i - distance, i) for i in devices if i - distance in devices]
    return lax.ppermute(block, axis, route)


def doubled(total, axis, bit):
    devices = range(lax.axis_size(axis))
    return total + lax.ppermute(total, axis, [(i, i ^ bit) for i in devices])


def total_of_all(totals, group):
    sizes = [lax.axis_size("row"), lax.axis_size("frame")]
    if any(size & (size - 1) for size in sizes):
        return lax.psum(totals, ("frame", "row"))
    bit = 1
    while bit < sizes[0]:
        totals = doubled(totals, "row", bit)
        bit *= 2
    bit = group
    while bit < sizes[1]:
        totals = doubled(totals, "frame", bit)
        bit *= 2
    parts = swap([totals] * group, group)
    while len(parts) > 1:
        parts = [parts[k] + parts[k + 1] for k in range(0, len(parts), 2)]
    return parts[0]


def shards(footage):
    frames, rows, width = footage.shape
    group = SPAN // frames
    top = shifted(footage[:, rows - HALO :], "row", 1)
    bottom = shifted(footage[:, :HALO], "row", -1)
    firsts, rest, coeffs = space(footage, top, bottom, group)
    firsts = swap(firsts, group)
    rest = [swap(r, group) for r in rest]
    power = None
    back = []
    for c in range(CHUNKS):
        to_right, to_left = edges(group, c, firsts, rest[c])
        left = shifted(to_right, "frame", group)
        right = shifted(to_left, "frame", -group)
        pieces, part_power = finish_time(group, c, firsts, rest[c], left, right)
        back.append(swap(pieces, group))
        power = part_power if power is None else power + part_power
    period = 2**SLEVELS
    column_phase = np.arange(width) % period
    selector = jnp.asarray((column_phase[:, None] == np.arange(period)[None, :]).astype(np.float32))
    pattern = jnp.dot(
        power.reshape((TLEVELS + 1) * SUB, width), selector, precision=lax.Precision.HIGHEST
    ).reshape(TLEVELS + 1, SUB * period)
    totals = jnp.dot(
        pattern, jnp.asarray(space_table(SLEVELS), jnp.float32), precision=lax.Precision.HIGHEST
    )
    totals = total_of_all(totals, group)
    for c in range(CHUNKS):
        coeffs = place(group, c, back[c], coeffs)
    means = band_means(
        totals,
        frames * lax.axis_size("frame"),
        rows * lax.axis_size("row"),
        width,
        SLEVELS,
        TLEVELS,
    )
    return (coeffs, means)


def solution(mesh):
    return jax.shard_map(
        shards,
        mesh=mesh,
        in_specs=(P("frame", "row", None),),
        out_specs=(P("frame", "row", None), P()),
        check_vma=False,
    )
```

```python
import functools

import jax
import jax.numpy as jnp
import numpy as np
from jax import lax
from jax.experimental import pallas as pl
from jax.experimental.pallas import tpu as pltpu
from jax.sharding import PartitionSpec as P


SLEVELS = 3
TLEVELS = 3

LIFT_ALPHA = -1.586134342
LIFT_BETA = -0.05298011854
LIFT_GAMMA = 0.8829110762
LIFT_DELTA = 0.4435068522
LIFT_ZETA = 1.149604398
FACTORS = (LIFT_ALPHA, LIFT_BETA, LIFT_GAMMA, LIFT_DELTA)

LANES = 128
SUB = 8
WIDE = 2 * LANES
TILE_ROWS = 384
HALO = 32
PAD = SUB
SPAN = 2 * 2**TLEVELS
KEPT = (0, 2, 3)


def level_of(number, ceiling):
    depth_now = 1
    while number % 2 == 0 and depth_now <= ceiling:
        number = number // 2
        depth_now = depth_now + 1
    return depth_now


def space_table(levels):
    period = 2**levels
    band_table = np.zeros((period * period, 3 * levels + 1), np.float32)
    for row_pos in range(period):
        for col_pos in range(period):
            row_level = level_of(row_pos, levels)
            col_level = level_of(col_pos, levels)
            finest = min(row_level, col_level)
            if finest > levels:
                column = 3 * levels
            elif row_level == col_level:
                column = 3 * (finest - 1) + 2
            elif row_level == finest:
                column = 3 * (finest - 1)
            else:
                column = 3 * (finest - 1) + 1
            band_table[row_pos * period + col_pos, column] = 1.0
    return band_table


def time_table(levels):
    period = 2**levels
    band_table = np.zeros((period, levels + 1), np.float32)
    for number in range(period):
        band_table[number, level_of(number, levels) - 1] = 1.0
    return band_table


def band_means(totals, frames_all, rows_all, cols_all, levels_s, levels_t):
    space_share = space_table(levels_s).sum(0) / float((2**levels_s) ** 2)
    time_share = time_table(levels_t).sum(0) / float(2**levels_t)
    counts = (
        float(frames_all) * float(rows_all) * float(cols_all) * np.outer(time_share, space_share)
    )
    return totals / jnp.asarray(counts, jnp.float32)


def lift_rows(buf, count):
    groups = count // SUB

    def step(odd, factor):
        target, near, far = (1, 0, 2) if odd else (0, -1, 1)

        def body(k, carry):
            top = PAD + 2 * SUB * k
            at = pl.ds(top + target, SUB, stride=2)
            for j in range(buf.shape[0]):
                buf[j, at, :] = buf[j, at, :] + factor * (
                    buf[j, pl.ds(top + near, SUB, stride=2), :]
                    + buf[j, pl.ds(top + far, SUB, stride=2), :]
                )
            return carry

        lax.fori_loop(0, groups, body, 0, unroll=5)

    step(True, LIFT_ALPHA)
    step(False, LIFT_BETA)
    step(True, LIFT_GAMMA)
    step(False, LIFT_DELTA)


def filter_taps():
    size = 8 * len(FACTORS)
    lifted = np.eye(size)
    for count, factor in enumerate(FACTORS):
        for n in range(1 - count % 2, size - 1, 2):
            lifted[n] += factor * (lifted[n - 1] + lifted[n + 1])
    middle = size // 2
    reach = len(FACTORS) + 1
    low = [lifted[middle, middle + k] * LIFT_ZETA for k in range(reach)]
    high = [lifted[middle + 1, middle + 1 + k] / LIFT_ZETA for k in range(reach)]
    return low, high


def column_weights(stride):
    low, high = filter_taps()
    band = np.zeros((WIDE + 2 * LANES, WIDE))
    for n in range(0, WIDE, stride):
        taps = low if n // stride % 2 == 0 else high
        for k, tap in enumerate(taps):
            band[LANES + n + k * stride, n] = tap
            band[LANES + n - k * stride, n] = tap
    upper = band.astype(jnp.bfloat16)
    lower = (band - upper.astype(np.float64)).astype(jnp.bfloat16)
    return np.concatenate([upper, lower])


def filter_cols(buf, rows, level, weights, split):
    blocks = buf.shape[0]
    stride = 2**level
    upper, lower = split
    lane = lax.broadcasted_iota(jnp.int32, (2 * SUB, LANES), 1)
    sub = lax.broadcasted_iota(jnp.int32, (2 * SUB, LANES), 0)
    scale = jnp.where(sub % 2 == 0, jnp.float32(LIFT_ZETA), jnp.float32(1.0 / LIFT_ZETA))
    before = (LANES - lane) % LANES
    after = (2 * LANES - 2 * stride - lane) % LANES

    def halves(i, carry):
        at = pl.ds(pl.multiple_of(2 * SUB * i, 2 * SUB), 2 * SUB)
        v = [buf[j, pl.ds(PAD + 2 * SUB * i, 2 * SUB), :] * scale for j in range(blocks)]
        left = jnp.take_along_axis(v[0], before, axis=1)
        right = jnp.take_along_axis(v[-1], after, axis=1)
        for j, x in enumerate([left] + v + [right]):
            c = slice(j * LANES, (j + 1) * LANES)
            top = x.astype(jnp.bfloat16)
            upper[at, c] = top
            lower[at, c] = (x - top.astype(jnp.float32)).astype(jnp.bfloat16)
        return carry

    lax.fori_loop(0, rows // (2 * SUB), halves, 0, unroll=5)
    depth = WIDE + 2 * LANES
    heavy, light = weights[level, :depth], weights[level, depth:]
    factor = jnp.concatenate([heavy, heavy, light])
    tile = min(rows, TILE_ROWS)
    across = blocks * LANES // WIDE

    def block(i, carry):
        r = pl.multiple_of(i // across * tile, SUB)
        n = i % across
        k = pl.ds(pl.multiple_of(n * WIDE, WIDE), depth)
        at = pl.ds(pl.multiple_of(r, 2 * SUB), tile)
        x, rest = upper[at, k], lower[at, k]
        y = jnp.dot(
            jnp.concatenate([x, rest, x], axis=1), factor, preferred_element_type=jnp.float32
        )
        for h in range(WIDE // LANES):
            buf[n * (WIDE // LANES) + h, pl.ds(PAD + r, tile), :] = y[:, h * LANES : (h + 1) * LANES]
        return carry

    lax.fori_loop(0, rows // tile * across, block, 0, unroll=4)


def spatial_frame(load, strip, rows, weights, scratch):
    bufs, split = scratch[:SLEVELS], scratch[SLEVELS:]
    row_index = lax.axis_index("row")
    is_first = row_index == 0
    is_last = row_index == lax.axis_size("row") - 1
    b = bufs[0]
    places = segment_places(strip)
    for at, (start, count) in zip(places, strip):
        first = PAD + at
        load(b, first - HALO, start - HALO, count + 2 * HALO)
        if start == 0:

            @pl.when(is_first)
            def _(first=first):
                for j in range(1, HALO):
                    b[:, first - j : first - j + 1, :] = b[:, first + j : first + j + 1, :]

    total = buffer_rows(strip)
    for level in range(SLEVELS):
        b = bufs[level]
        stride = 2**level
        for at, (start, count) in zip(places, strip):
            if start + count == rows:

                @pl.when(is_last)
                def _(b=b, stop=PAD + (at + count) // stride, level=level):
                    inner = HALO // 2**level
                    for j in range(inner - 1 if level == 0 else inner * 5 // 8):
                        b[:, stop + j : stop + j + 1, :] = b[:, stop - 2 - j : stop - 1 - j, :]

        lift_rows(b, total // stride // 2)
        filter_cols(b, total // stride, level, weights, split)
        if level + 1 < SLEVELS:
            low = bufs[level + 1]

            def body(k, carry, b=b, low=low):
                for j in range(b.shape[0]):
                    low[j, pl.ds(PAD + SUB * k, SUB), :] = b[
                        j, pl.ds(PAD + 2 * SUB * k, SUB, stride=2), :
                    ]
                return carry

            lax.fori_loop(0, total // stride // 2 // SUB, body, 0, unroll=5)
    lane = lax.broadcasted_iota(jnp.int32, (SUB, LANES), 1)
    for level in reversed(range(SLEVELS - 1)):
        b, low = bufs[level], bufs[level + 1]
        stride = 2 ** (level + 1)
        keep = lane % stride == 0
        for at, (_, count) in zip(places, strip):

            def body(k, carry, b=b, low=low, keep=keep, stride=stride, at=at):
                outer = pl.ds(PAD + at // (stride // 2) + 2 * SUB * k, SUB, stride=2)
                inner = pl.ds(PAD + at // stride + SUB * k, SUB)
                for j in range(b.shape[0]):
                    b[j, outer, :] = jnp.where(keep, low[j, inner, :], b[j, outer, :])
                return carry

            lax.fori_loop(0, count // stride // SUB, body, 0, unroll=4)


def strips_of(rows):
    edge = rows // 4
    return [[(edge, rows - 2 * edge)], [(0, edge), (rows - edge, edge)]]


def strip_rows(strip):
    return sum(count for _, count in strip)


def buffer_rows(strip):
    return sum(count + 2 * HALO for _, count in strip)


def segment_places(strip):
    places, at = [], 0
    for _, count in strip:
        places.append(at + HALO)
        at += count + 2 * HALO
    return places


def part_start(starts, strip, owner, group):
    part = strip_rows(strip) // group
    where = owner * part + starts[0]
    passed = 0
    for k in range(1, len(strip)):
        passed += strip[k - 1][1]
        where = jnp.where(owner * part >= passed, owner * part - passed + starts[k], where)
    return where


def member(group):
    return lax.axis_index("frame") % group


UNITS = ((0, (0,)), (0, (1,)), (0, (2, 3)), (1, (0, 1)), (1, (2, 3)))


def turns_of(strips, group):
    middle = strip_rows(strips[0]) // group
    outer = strip_rows(strips[1]) // group
    return [(0, 0, middle), (1, 0, outer // 2), (1, outer // 2, outer // 2)]


def space_kernel(group, strip, rows, *refs):
    inner = all(start > 0 and start + count < rows for start, count in strip)
    x_ref = refs[0].at[0]
    top_ref, bottom_ref = (None, None) if inner else (refs[1].at[0], refs[2].at[0])
    refs = refs[1:] if inner else refs[3:]
    weights, pieces, scratch = refs[0], refs[1 : 1 + group], refs[1 + group :]

    def load(b, to, start, count):
        spans = []
        if start < 0:
            spans.append((top_ref, 0, HALO, to))
            start, count, to = start + HALO, count - HALO, to + HALO
        if start + count > rows:
            spans.append((bottom_ref, 0, HALO, to + count - HALO))
            count -= HALO
        spans.append((x_ref, start, count, to))
        for j in range(b.shape[0]):
            c = slice(j * LANES, (j + 1) * LANES)
            for source, begin, length, place in spans:
                b[j, place : place + length, :] = source[begin : begin + length, c]

    spatial_frame(load, strip, rows, weights, scratch)
    me = member(group)
    part = strip_rows(strip) // group
    starts = [PAD + at for at in segment_places(strip)]
    for d in range(group):
        start = pl.multiple_of(part_start(starts, strip, me ^ d, group), SUB)
        for j in range(scratch[0].shape[0]):
            c = slice(j * LANES, (j + 1) * LANES)
            pieces[d][0, :, c] = scratch[0][j, pl.ds(start, part), :]


def space(unit, footage, top, bottom, weights, strips, group):
    which, chosen = UNITS[unit]
    strip = strips[which]
    _, rows, width = footage.shape
    part = strip_rows(strip) // group
    total = buffer_rows(strip)
    f32 = jnp.float32
    shift = chosen[0]

    def frame(height):
        return pl.BlockSpec((1, height, width), lambda g: (g + shift, 0, 0))

    inner = all(start > 0 and start + count < rows for start, count in strip)
    given = [footage] if inner else [footage, top, bottom]
    specs = [frame(rows)] if inner else [frame(rows), frame(HALO), frame(HALO)]
    shapes = [
        pltpu.VMEM((width // LANES, total // 2**level + 2 * PAD, LANES), f32)
        for level in range(SLEVELS)
    ] + [pltpu.VMEM((total, width + 2 * LANES), jnp.bfloat16)] * 2
    return pl.pallas_call(
        functools.partial(space_kernel, group, strip, rows),
        grid=(len(chosen),),
        in_specs=specs + [pl.BlockSpec(weights.shape, lambda g: (0, 0, 0))],
        out_specs=[pl.BlockSpec((1, part, width), lambda g: (g, 0, 0))] * group,
        out_shape=[jax.ShapeDtypeStruct((len(chosen), part, width), f32)] * group,
        scratch_shapes=shapes,
        cost_estimate=pl.CostEstimate(
            flops=len(chosen) * rows * width * 400,
            bytes_accessed=len(chosen) * rows * width * 8,
            transcendentals=0,
        ),
    )(*given, weights)


BLOCK_ROWS = 32


def each_member(group, body):
    me = member(group)
    for place in range(group):
        pl.when(me == place)(functools.partial(body, place))


def span_of(group, chosen, refs, place):
    frames = SPAN // group
    found = []
    for n in range(SPAN):
        d, f = place ^ (n // frames), n % frames
        u = [f in own for own in chosen].index(True)
        found.append((refs[u * group + d], chosen[u].index(f)))
    return found


def each_tile(rows, width, body):
    tiles = width // WIDE

    def step(k, carry):
        r = pl.multiple_of((k // tiles) * SUB, SUB)
        c = pl.multiple_of((k % tiles) * WIDE, WIDE)
        body(pl.ds(r, SUB), pl.ds(c, WIDE))
        return carry

    lax.fori_loop(0, rows // SUB * tiles, step, 0)


def partial_levels(x):
    o = {n: x[n] - 0.5 * (x[n - 1] + x[n + 1]) for n in range(1, SPAN - 1, 2)}
    o[15] = x[15] - 0.5 * x[14]
    low = {n: x[n] + 0.25 * (o[n - 1] + o[n + 1]) for n in range(2, SPAN, 2)}
    low[0] = x[0] + 0.25 * o[1]
    p = {n: low[n] - 0.5 * (low[n - 2] + low[n + 2]) for n in (2, 6, 10)}
    p[14] = low[14] - 0.5 * low[12]
    m = {n: low[n] + 0.25 * (p[n - 2] + p[n + 2]) for n in (8, 12)}
    m[0] = low[0] + 0.25 * p[2]
    q12 = m[12] - 0.5 * m[8]
    to_right = (o[15], p[14], q12)
    to_left = (x[0], low[0], m[0])
    return to_right, to_left


def full_levels(x, left, right, is_first, is_last):
    a0, b0, c0 = left
    x16, low16, m16 = right
    o = {n: x[n] - 0.5 * (x[n - 1] + x[n + 1]) for n in range(1, SPAN - 1, 2)}
    o[15] = x[15] - 0.5 * (x[14] + jnp.where(is_last, x[14], x16))
    before = jnp.where(is_first, o[1], a0 - 0.5 * x[0])
    low = {n: x[n] + 0.25 * (o[n - 1] + o[n + 1]) for n in range(2, SPAN, 2)}
    low[0] = x[0] + 0.25 * (before + o[1])
    p = {n: low[n] - 0.5 * (low[n - 2] + low[n + 2]) for n in (2, 6, 10)}
    p[14] = low[14] - 0.5 * (low[12] + jnp.where(is_last, low[12], low16 + 0.25 * o[15]))
    before = jnp.where(is_first, p[2], b0 - 0.125 * x[0] - 0.5 * low[0])
    m = {n: low[n] + 0.25 * (p[n - 2] + p[n + 2]) for n in (4, 8, 12)}
    m[0] = low[0] + 0.25 * (before + p[2])
    q4 = m[4] - 0.5 * (m[0] + m[8])
    after = jnp.where(is_last, m[8], m16 + 0.21875 * o[15] + 0.25 * p[14])
    q12 = m[12] - 0.5 * (m[8] + after)
    before = jnp.where(is_first, q4, c0 - 0.03125 * x[0] - 0.125 * low[0] - 0.5 * m[0])
    y = dict(o)
    y.update(p)
    y[4] = q4
    y[12] = q12
    y[0] = m[0] + 0.25 * (before + q4)
    y[8] = m[8] + 0.25 * (q4 + q12)
    return [y[n] for n in range(SPAN)]


def edges_kernel(group, chosen, *refs):
    given = len(chosen) * group
    to_right, to_left = refs[given:]
    _, rows, width = to_right.shape

    def variant(place):
        span = span_of(group, chosen, refs[:given], place)

        def body(r, c):
            right, left = partial_levels([ref[k, r, c] for ref, k in span])
            for k in range(TLEVELS):
                to_right[k, r, c] = right[k]
                to_left[k, r, c] = left[k]

        each_tile(rows, width, body)

    each_member(group, variant)


def time_kernel(group, chosen, *refs):
    given = len(chosen) * group
    left, right = refs[given : given + 2]
    pieces = refs[given + 2 : given + 2 + group]
    power = refs[given + 2 + group]
    frames = SPAN // group
    _, rows, width = left.shape
    spot = lax.axis_index("frame") // group
    is_first = spot == 0
    is_last = spot == lax.axis_size("frame") // group - 1

    @pl.when(pl.program_id(0) == 0)
    def _():
        power[...] = jnp.zeros_like(power)

    def variant(place):
        span = span_of(group, chosen, refs[:given], place)

        def body(r, c):
            y = full_levels(
                [ref[k, r, c] for ref, k in span],
                [left[k, r, c] for k in range(TLEVELS)],
                [right[k, r, c] for k in range(TLEVELS)],
                is_first,
                is_last,
            )
            sums = [None] * (TLEVELS + 1)
            for n in range(SPAN):
                t = level_of(n % 2**TLEVELS, TLEVELS) - 1
                square = y[n] * y[n]
                sums[t] = square if sums[t] is None else sums[t] + square
                if n % frames in KEPT:
                    pieces[place ^ (n // frames)][KEPT.index(n % frames), r, c] = y[n]
            for t in range(TLEVELS + 1):
                power[t, :, c] = power[t, :, c] + sums[t]

        each_tile(rows, width, body)

    each_member(group, variant)


def span_specs(group, chosen, first, width):
    skip = first // BLOCK_ROWS
    return [
        pl.BlockSpec((len(frames), BLOCK_ROWS, width), lambda i: (0, skip + i, 0))
        for frames in chosen
        for _ in range(group)
    ]


def time_cost(rows, width, frames):
    return pl.CostEstimate(
        flops=rows * width * 2000, bytes_accessed=rows * width * 4 * frames, transcendentals=0
    )


def edges(group, first, rows, chosen, given):
    width = given[0].shape[2]
    spec = pl.BlockSpec((TLEVELS, BLOCK_ROWS, width), lambda i: (0, i, 0))
    shape = jax.ShapeDtypeStruct((TLEVELS, rows, width), jnp.float32)
    return pl.pallas_call(
        functools.partial(edges_kernel, group, chosen),
        grid=(rows // BLOCK_ROWS,),
        in_specs=span_specs(group, chosen, first, width),
        out_specs=[spec, spec],
        out_shape=[shape, shape],
        cost_estimate=time_cost(rows, width, SPAN + 6),
    )(*given)


def finish_time(group, first, rows, chosen, given, left, right):
    width = given[0].shape[2]
    kept = len(KEPT)
    halo = pl.BlockSpec((TLEVELS, BLOCK_ROWS, width), lambda i: (0, i, 0))
    outs = pl.pallas_call(
        functools.partial(time_kernel, group, chosen),
        grid=(rows // BLOCK_ROWS,),
        in_specs=span_specs(group, chosen, first, width) + [halo, halo],
        out_specs=[pl.BlockSpec((kept, BLOCK_ROWS, width), lambda i: (0, i, 0))] * group
        + [pl.BlockSpec((TLEVELS + 1, SUB, width), lambda i: (0, 0, 0))],
        out_shape=[jax.ShapeDtypeStruct((kept, rows, width), jnp.float32)] * group
        + [jax.ShapeDtypeStruct((TLEVELS + 1, SUB, width), jnp.float32)],
        cost_estimate=time_cost(rows, width, 2 * SPAN + 6),
    )(*given, left, right)
    return outs[:group], outs[group]


def home_kernel(group, strip, fresh, *refs):
    given = 3 * group
    out, held, sems = refs[given if fresh else given + 1 :]
    me = member(group)
    starts = [start for start, _ in strip]
    step = pl.program_id(0)

    def copy(d, at):
        start = part_start(starts, strip, me ^ d, group) + at * BLOCK_ROWS
        return pltpu.make_async_copy(
            held.at[at, d],
            out.at[1, pl.ds(pl.multiple_of(start, SUB), BLOCK_ROWS)],
            sems.at[at, d],
        )

    for d in range(group):
        held[step, d] = refs[group + d][0] - 0.5 * (refs[d][0] + refs[2 * group + d][0])
        copy(d, step).start()

    @pl.when(step == held.shape[0] - 1)
    def _():
        for at in range(held.shape[0]):
            for d in range(group):
                copy(d, at).wait()


def home(group, strip, chosen, sent, shape, coeffs):
    width = shape[2]
    part = strip_rows(strip) // group
    given, specs = [], []
    for f in range(3):
        u = [f in frames for frames in chosen].index(True)
        k = chosen[u].index(f)
        given += sent[u]
        specs += [pl.BlockSpec((1, BLOCK_ROWS, width), lambda i, k=k: (k, i, 0))] * group
    fresh = coeffs is None
    if not fresh:
        given.append(coeffs)
        specs.append(pl.BlockSpec(memory_space=pl.ANY))
    return pl.pallas_call(
        functools.partial(home_kernel, group, strip, fresh),
        grid=(part // BLOCK_ROWS,),
        in_specs=specs,
        out_specs=pl.BlockSpec(memory_space=pl.ANY),
        out_shape=jax.ShapeDtypeStruct(shape, jnp.float32),
        input_output_aliases={} if fresh else {3 * group: 0},
        scratch_shapes=[
            pltpu.VMEM((part // BLOCK_ROWS, group, BLOCK_ROWS, width), jnp.float32),
            pltpu.SemaphoreType.DMA((part // BLOCK_ROWS, group)),
        ],
        cost_estimate=time_cost(part, width, 4 * group),
    )(*given)


def place_kernel(group, strip, first, *refs):
    pieces, _, out, held, ins, outs = refs[:group], *refs[group:]
    kept, rows, _ = pieces[0].shape
    me = member(group)
    starts = [start for start, _ in strip]
    arriving, leaving = [], []
    for d in range(group):
        start = pl.multiple_of(part_start(starts, strip, me ^ d, group) + first, SUB)
        for k, f in enumerate(KEPT):
            n = d * kept + k
            arriving.append(pltpu.make_async_copy(pieces[d].at[k], held.at[n], ins.at[n]))
            leaving.append(
                pltpu.make_async_copy(held.at[n], out.at[f, pl.ds(start, rows)], outs.at[n])
            )
    for copy in arriving:
        copy.start()
    for copy, after in zip(arriving, leaving):
        copy.wait()
        after.start()
    for copy in leaving:
        copy.wait()


def place(group, strip, first, pieces, coeffs):
    kept, rows, width = pieces[0].shape
    count = group * kept
    return pl.pallas_call(
        functools.partial(place_kernel, group, strip, first),
        in_specs=[pl.BlockSpec(memory_space=pl.ANY)] * (group + 1),
        out_specs=pl.BlockSpec(memory_space=pl.ANY),
        out_shape=jax.ShapeDtypeStruct(coeffs.shape, coeffs.dtype),
        input_output_aliases={group: 0},
        scratch_shapes=[
            pltpu.VMEM((count, rows, width), jnp.float32),
            pltpu.SemaphoreType.DMA((count,)),
            pltpu.SemaphoreType.DMA((count,)),
        ],
        cost_estimate=time_cost(rows, width, 2 * count),
    )(*pieces, coeffs)


def swap(blocks, group):
    devices = range(lax.axis_size("frame"))
    out = [blocks[0]]
    for d in range(1, group):
        out.append(lax.ppermute(blocks[d], "frame", [(i, i ^ d) for i in devices]))
    return out


def shifted(block, axis, distance):
    devices = range(lax.axis_size(axis))
    route = [(i - distance, i) for i in devices if i - distance in devices]
    return lax.ppermute(block, axis, route)


def doubled(total, axis, bit):
    devices = range(lax.axis_size(axis))
    return total + lax.ppermute(total, axis, [(i, i ^ bit) for i in devices])


def total_of_all(totals, group):
    sizes = [lax.axis_size("row"), lax.axis_size("frame")]
    if any(size & (size - 1) for size in sizes):
        return lax.psum(totals, ("frame", "row"))
    bit = 1
    while bit < sizes[0]:
        totals = doubled(totals, "row", bit)
        bit *= 2
    bit = group
    while bit < sizes[1]:
        totals = doubled(totals, "frame", bit)
        bit *= 2
    parts = swap([totals] * group, group)
    while len(parts) > 1:
        parts = [parts[k] + parts[k + 1] for k in range(0, len(parts), 2)]
    return parts[0]


def shards(footage):
    frames, rows, width = footage.shape
    group = SPAN // frames
    strips = strips_of(rows)
    weights = jnp.asarray(np.stack([column_weights(2**level) for level in range(SLEVELS)]))
    top = shifted(footage[:, rows - HALO :], "row", 1)
    bottom = shifted(footage[:, :HALO], "row", -1)
    sent, arrived, chosen = [[], []], [[], []], [[], []]
    for u, (which, own) in enumerate(UNITS):
        pieces = space(u, footage, top, bottom, weights, strips, group)
        sent[which].append(pieces)
        chosen[which].append(own)
        arrived[which] += swap(pieces, group)
    coeffs = None
    for which, strip in enumerate(strips):
        coeffs = home(group, strip, chosen[which], sent[which], footage.shape, coeffs)
    power = None
    back = []
    turns = turns_of(strips, group)
    for which, first, count in turns:
        given, own = arrived[which], chosen[which]
        to_right, to_left = edges(group, first, count, own, given)
        left = shifted(to_right, "frame", group)
        right = shifted(to_left, "frame", -group)
        pieces, part_power = finish_time(group, first, count, own, given, left, right)
        back.append(swap(pieces, group))
        power = part_power if power is None else power + part_power
    period = 2**SLEVELS
    column_phase = np.arange(width) % period
    selector = jnp.asarray((column_phase[:, None] == np.arange(period)[None, :]).astype(np.float32))
    pattern = jnp.dot(
        power.reshape((TLEVELS + 1) * SUB, width), selector, precision=lax.Precision.HIGHEST
    ).reshape(TLEVELS + 1, SUB * period)
    totals = jnp.dot(
        pattern, jnp.asarray(space_table(SLEVELS), jnp.float32), precision=lax.Precision.HIGHEST
    )
    totals = total_of_all(totals, group)
    for t, (which, first, _) in enumerate(turns):
        coeffs = place(group, strips[which], first, back[t], coeffs)
    means = band_means(
        totals,
        frames * lax.axis_size("frame"),
        rows * lax.axis_size("row"),
        width,
        SLEVELS,
        TLEVELS,
    )
    return (coeffs, means)


def solution(mesh):
    return jax.shard_map(
        shards,
        mesh=mesh,
        in_specs=(P("frame", "row", None),),
        out_specs=(P("frame", "row", None), P()),
        check_vma=False,
    )
```

```python
import functools

import jax
import jax.numpy as jnp
import numpy as np
from jax import lax
from jax.experimental import pallas as pl
from jax.experimental.pallas import tpu as pltpu
from jax.sharding import PartitionSpec as P


SLEVELS = 3
TLEVELS = 3

LIFT_ALPHA = -1.586134342
LIFT_BETA = -0.05298011854
LIFT_GAMMA = 0.8829110762
LIFT_DELTA = 0.4435068522
LIFT_ZETA = 1.149604398
FACTORS = (LIFT_ALPHA, LIFT_BETA, LIFT_GAMMA, LIFT_DELTA)

LANES = 128
SUB = 8
WIDE = 2 * LANES
TILE_ROWS = 384
HALO = 32
PAD = SUB
SPAN = 2 * 2**TLEVELS
KEPT = (0, 2, 3)


def level_of(number, ceiling):
    depth_now = 1
    while number % 2 == 0 and depth_now <= ceiling:
        number = number // 2
        depth_now = depth_now + 1
    return depth_now


def space_table(levels):
    period = 2**levels
    band_table = np.zeros((period * period, 3 * levels + 1), np.float32)
    for row_pos in range(period):
        for col_pos in range(period):
            row_level = level_of(row_pos, levels)
            col_level = level_of(col_pos, levels)
            finest = min(row_level, col_level)
            if finest > levels:
                column = 3 * levels
            elif row_level == col_level:
                column = 3 * (finest - 1) + 2
            elif row_level == finest:
                column = 3 * (finest - 1)
            else:
                column = 3 * (finest - 1) + 1
            band_table[row_pos * period + col_pos, column] = 1.0
    return band_table


def time_table(levels):
    period = 2**levels
    band_table = np.zeros((period, levels + 1), np.float32)
    for number in range(period):
        band_table[number, level_of(number, levels) - 1] = 1.0
    return band_table


def band_means(totals, frames_all, rows_all, cols_all, levels_s, levels_t):
    space_share = space_table(levels_s).sum(0) / float((2**levels_s) ** 2)
    time_share = time_table(levels_t).sum(0) / float(2**levels_t)
    counts = (
        float(frames_all) * float(rows_all) * float(cols_all) * np.outer(time_share, space_share)
    )
    return totals / jnp.asarray(counts, jnp.float32)


def times(count, body):
    unroll = next(u for u in (6, 5, 4, 3, 2, 1) if count % u == 0)
    lax.fori_loop(0, count, body, 0, unroll=unroll)


def lift_rows(buf, count):
    groups = count // SUB

    def step(odd, factor):
        target, near, far = (1, 0, 2) if odd else (0, -1, 1)

        def body(k, carry):
            top = PAD + 2 * SUB * k
            at = pl.ds(top + target, SUB, stride=2)
            for j in range(buf.shape[0]):
                buf[j, at, :] = buf[j, at, :] + factor * (
                    buf[j, pl.ds(top + near, SUB, stride=2), :]
                    + buf[j, pl.ds(top + far, SUB, stride=2), :]
                )
            return carry

        times(groups, body)

    step(True, LIFT_ALPHA)
    step(False, LIFT_BETA)
    step(True, LIFT_GAMMA)
    step(False, LIFT_DELTA)


def filter_taps():
    size = 8 * len(FACTORS)
    lifted = np.eye(size)
    for count, factor in enumerate(FACTORS):
        for n in range(1 - count % 2, size - 1, 2):
            lifted[n] += factor * (lifted[n - 1] + lifted[n + 1])
    middle = size // 2
    reach = len(FACTORS) + 1
    low = [lifted[middle, middle + k] * LIFT_ZETA for k in range(reach)]
    high = [lifted[middle + 1, middle + 1 + k] / LIFT_ZETA for k in range(reach)]
    return low, high


def column_weights(stride):
    low, high = filter_taps()
    band = np.zeros((WIDE + 2 * LANES, WIDE))
    for n in range(0, WIDE, stride):
        taps = low if n // stride % 2 == 0 else high
        for k, tap in enumerate(taps):
            band[LANES + n + k * stride, n] = tap
            band[LANES + n - k * stride, n] = tap
    heavy = band.astype(jnp.bfloat16)
    light = (band - heavy.astype(np.float64)).astype(jnp.bfloat16)
    own = slice(LANES, LANES + WIDE)
    half, quarter = LANES // 2, LANES // 4

    def sides(part):
        return np.concatenate([part[LANES + WIDE :][:half], part[:LANES][half:]])

    packed = sides(heavy)
    packed = np.concatenate(
        [
            packed[:quarter],
            packed[3 * quarter :],
            packed[:quarter],
            packed[3 * quarter :],
        ]
    )
    return np.concatenate([heavy[own], light[own], packed, sides(light)])


def filter_cols(buf, rows, level, weights, split):
    blocks = buf.shape[0]
    stride = 2**level
    upper, lower, beside = split
    lane = lax.broadcasted_iota(jnp.int32, (2 * SUB, LANES), 1)
    sub = lax.broadcasted_iota(jnp.int32, (2 * SUB, LANES), 0)
    scale = jnp.where(sub % 2 == 0, jnp.float32(LIFT_ZETA), jnp.float32(1.0 / LIFT_ZETA))
    before = (LANES - lane) % LANES
    after = (2 * LANES - 2 * stride - lane) % LANES
    right_half = lane < LANES // 2
    outer = (lane < LANES // 4) | (lane >= 3 * LANES // 4)
    wide = WIDE // LANES

    def halves(i, carry):
        at = pl.ds(pl.multiple_of(2 * SUB * i, 2 * SUB), 2 * SUB)
        v = [buf[j, pl.ds(PAD + 2 * SUB * i, 2 * SUB), :] * scale for j in range(blocks)]
        left = jnp.take_along_axis(v[0], before, axis=1)
        right = jnp.take_along_axis(v[-1], after, axis=1)
        for j, x in enumerate(v):
            c = slice(j * LANES, (j + 1) * LANES)
            top = x.astype(jnp.bfloat16)
            upper[at, c] = top
            lower[at, c] = (x - top.astype(jnp.float32)).astype(jnp.bfloat16)
        for n in range(blocks // wide):
            j = n * wide
            x = jnp.where(
                right_half,
                right if j + wide == blocks else v[j + wide],
                left if n == 0 else v[j - 1],
            )
            top = x.astype(jnp.bfloat16)
            rest = pltpu.roll(x - top.astype(jnp.float32), LANES // 2, 1)
            beside[at, 2 * n * LANES : (2 * n + 1) * LANES] = jnp.where(
                outer, top.astype(jnp.float32), rest
            ).astype(jnp.bfloat16)
            beside[at, (2 * n + 1) * LANES : (2 * n + 2) * LANES] = top
        return carry

    times(rows // (2 * SUB), halves)
    heavy, light, sides = (weights[level, k * WIDE : (k + 1) * WIDE] for k in range(3))
    factor = jnp.concatenate([heavy, heavy, light, sides])
    tile = min(rows, TILE_ROWS)
    across = blocks * LANES // WIDE

    def block(i, carry):
        r = pl.multiple_of(i // across * tile, SUB)
        n = i % across
        k = pl.ds(pl.multiple_of(n * WIDE, WIDE), WIDE)
        side = pl.ds(pl.multiple_of(2 * n * LANES, LANES), 2 * LANES)
        at = pl.ds(pl.multiple_of(r, 2 * SUB), tile)
        x, rest = upper[at, k], lower[at, k]
        y = jnp.dot(
            jnp.concatenate([x, rest, x, beside[at, side]], axis=1),
            factor,
            preferred_element_type=jnp.float32,
        )
        for h in range(WIDE // LANES):
            buf[n * (WIDE // LANES) + h, pl.ds(PAD + r, tile), :] = y[:, h * LANES : (h + 1) * LANES]
        return carry

    lax.fori_loop(0, rows // tile * across, block, 0, unroll=4)


def spatial_frame(load, strip, rows, weights, scratch):
    bufs, split = scratch[:SLEVELS], scratch[SLEVELS:]
    row_index = lax.axis_index("row")
    is_first = row_index == 0
    is_last = row_index == lax.axis_size("row") - 1
    b = bufs[0]
    places = segment_places(strip)
    for at, (start, count) in zip(places, strip):
        first = PAD + at
        load(b, first - HALO, start - HALO, count + 2 * HALO)
        if start == 0:

            @pl.when(is_first)
            def _(first=first):
                for j in range(1, HALO):
                    b[:, first - j : first - j + 1, :] = b[:, first + j : first + j + 1, :]

    total = buffer_rows(strip)
    for level in range(SLEVELS):
        b = bufs[level]
        stride = 2**level
        for at, (start, count) in zip(places, strip):
            if start + count == rows:

                @pl.when(is_last)
                def _(b=b, stop=PAD + (at + count) // stride, level=level):
                    inner = HALO // 2**level
                    for j in range(inner - 1 if level == 0 else inner * 5 // 8):
                        b[:, stop + j : stop + j + 1, :] = b[:, stop - 2 - j : stop - 1 - j, :]

        lift_rows(b, total // stride // 2)
        filter_cols(b, total // stride, level, weights, split)
        if level + 1 < SLEVELS:
            low = bufs[level + 1]

            def body(k, carry, b=b, low=low):
                for j in range(b.shape[0]):
                    low[j, pl.ds(PAD + SUB * k, SUB), :] = b[
                        j, pl.ds(PAD + 2 * SUB * k, SUB, stride=2), :
                    ]
                return carry

            times(total // stride // 2 // SUB, body)
    lane = lax.broadcasted_iota(jnp.int32, (SUB, LANES), 1)
    for level in reversed(range(SLEVELS - 1)):
        b, low = bufs[level], bufs[level + 1]
        stride = 2 ** (level + 1)
        keep = lane % stride == 0
        for at, (_, count) in zip(places, strip):

            def body(k, carry, b=b, low=low, keep=keep, stride=stride, at=at):
                outer = pl.ds(PAD + at // (stride // 2) + 2 * SUB * k, SUB, stride=2)
                inner = pl.ds(PAD + at // stride + SUB * k, SUB)
                for j in range(b.shape[0]):
                    b[j, outer, :] = jnp.where(keep, low[j, inner, :], b[j, outer, :])
                return carry

            times(count // stride // SUB, body)


def strips_of(rows):
    edge = rows // 4
    return [[(edge, rows - 2 * edge)], [(0, edge), (rows - edge, edge)]]


def strip_rows(strip):
    return sum(count for _, count in strip)


def buffer_rows(strip):
    return sum(count + 2 * HALO for _, count in strip)


def segment_places(strip):
    places, at = [], 0
    for _, count in strip:
        places.append(at + HALO)
        at += count + 2 * HALO
    return places


def part_start(starts, strip, owner, group):
    part = strip_rows(strip) // group
    where = owner * part + starts[0]
    passed = 0
    for k in range(1, len(strip)):
        passed += strip[k - 1][1]
        where = jnp.where(owner * part >= passed, owner * part - passed + starts[k], where)
    return where


def member(group):
    return lax.axis_index("frame") % group


UNITS = ((0, (0, 1)), (0, (2, 3)), (1, (0, 1)), (1, (2, 3)))


def turns_of(strips, group):
    middle = strip_rows(strips[0]) // group
    outer = strip_rows(strips[1]) // group
    return [
        (0, 0, middle // 2),
        (0, middle // 2, middle // 2),
        (1, 0, outer // 2),
        (1, outer // 2, outer // 2),
    ]


def space_kernel(group, strip, rows, *refs):
    inner = all(start > 0 and start + count < rows for start, count in strip)
    x_ref = refs[0].at[0]
    top_ref, bottom_ref = (None, None) if inner else (refs[1].at[0], refs[2].at[0])
    refs = refs[1:] if inner else refs[3:]
    weights, pieces, scratch = refs[0], refs[1 : 1 + group], refs[1 + group :]

    def load(b, to, start, count):
        spans = []
        if start < 0:
            spans.append((top_ref, 0, HALO, to))
            start, count, to = start + HALO, count - HALO, to + HALO
        if start + count > rows:
            spans.append((bottom_ref, 0, HALO, to + count - HALO))
            count -= HALO
        spans.append((x_ref, start, count, to))
        for j in range(b.shape[0]):
            c = slice(j * LANES, (j + 1) * LANES)
            for source, begin, length, place in spans:
                b[j, place : place + length, :] = source[begin : begin + length, c]

    spatial_frame(load, strip, rows, weights, scratch)
    me = member(group)
    part = strip_rows(strip) // group
    starts = [PAD + at for at in segment_places(strip)]
    for d in range(group):
        start = pl.multiple_of(part_start(starts, strip, me ^ d, group), SUB)
        for j in range(scratch[0].shape[0]):
            c = slice(j * LANES, (j + 1) * LANES)
            pieces[d][0, :, c] = scratch[0][j, pl.ds(start, part), :]


def space(unit, footage, top, bottom, weights, strips, group):
    which, chosen = UNITS[unit]
    strip = strips[which]
    _, rows, width = footage.shape
    part = strip_rows(strip) // group
    total = buffer_rows(strip)
    f32 = jnp.float32
    shift = chosen[0]

    def frame(height):
        return pl.BlockSpec((1, height, width), lambda g: (g + shift, 0, 0))

    inner = all(start > 0 and start + count < rows for start, count in strip)
    given = [footage] if inner else [footage, top, bottom]
    specs = [frame(rows)] if inner else [frame(rows), frame(HALO), frame(HALO)]
    shapes = [
        pltpu.VMEM((width // LANES, total // 2**level + 2 * PAD, LANES), f32)
        for level in range(SLEVELS)
    ] + [pltpu.VMEM((total, width), jnp.bfloat16)] * 3
    return pl.pallas_call(
        functools.partial(space_kernel, group, strip, rows),
        grid=(len(chosen),),
        in_specs=specs + [pl.BlockSpec(weights.shape, lambda g: (0, 0, 0))],
        out_specs=[pl.BlockSpec((1, part, width), lambda g: (g, 0, 0))] * group,
        out_shape=[jax.ShapeDtypeStruct((len(chosen), part, width), f32)] * group,
        scratch_shapes=shapes,
        cost_estimate=pl.CostEstimate(
            flops=len(chosen) * rows * width * 400,
            bytes_accessed=len(chosen) * rows * width * 8,
            transcendentals=0,
        ),
    )(*given, weights)


MOST_ROWS = 32


def each_member(group, body):
    me = member(group)
    for place in range(group):
        pl.when(me == place)(functools.partial(body, place))


def span_of(group, chosen, refs, place):
    frames = SPAN // group
    found = []
    for n in range(SPAN):
        d, f = place ^ (n // frames), n % frames
        u = [f in own for own in chosen].index(True)
        found.append((refs[u * group + d], chosen[u].index(f)))
    return found


def each_tile(rows, width, body):
    tiles = width // WIDE

    def step(k, carry):
        r = pl.multiple_of((k // tiles) * SUB, SUB)
        c = pl.multiple_of((k % tiles) * WIDE, WIDE)
        body(pl.ds(r, SUB), pl.ds(c, WIDE))
        return carry

    lax.fori_loop(0, rows // SUB * tiles, step, 0)


def partial_levels(x):
    o = {n: x[n] - 0.5 * (x[n - 1] + x[n + 1]) for n in range(1, SPAN - 1, 2)}
    o[15] = x[15] - 0.5 * x[14]
    low = {n: x[n] + 0.25 * (o[n - 1] + o[n + 1]) for n in range(2, SPAN, 2)}
    low[0] = x[0] + 0.25 * o[1]
    p = {n: low[n] - 0.5 * (low[n - 2] + low[n + 2]) for n in (2, 6, 10)}
    p[14] = low[14] - 0.5 * low[12]
    m = {n: low[n] + 0.25 * (p[n - 2] + p[n + 2]) for n in (8, 12)}
    m[0] = low[0] + 0.25 * p[2]
    q12 = m[12] - 0.5 * m[8]
    to_right = (o[15], p[14], q12)
    to_left = (x[0], low[0], m[0])
    return to_right, to_left


def full_levels(x, left, right, is_first, is_last):
    a0, b0, c0 = left
    x16, low16, m16 = right
    o = {n: x[n] - 0.5 * (x[n - 1] + x[n + 1]) for n in range(1, SPAN - 1, 2)}
    o[15] = x[15] - 0.5 * (x[14] + jnp.where(is_last, x[14], x16))
    before = jnp.where(is_first, o[1], a0 - 0.5 * x[0])
    low = {n: x[n] + 0.25 * (o[n - 1] + o[n + 1]) for n in range(2, SPAN, 2)}
    low[0] = x[0] + 0.25 * (before + o[1])
    p = {n: low[n] - 0.5 * (low[n - 2] + low[n + 2]) for n in (2, 6, 10)}
    p[14] = low[14] - 0.5 * (low[12] + jnp.where(is_last, low[12], low16 + 0.25 * o[15]))
    before = jnp.where(is_first, p[2], b0 - 0.125 * x[0] - 0.5 * low[0])
    m = {n: low[n] + 0.25 * (p[n - 2] + p[n + 2]) for n in (4, 8, 12)}
    m[0] = low[0] + 0.25 * (before + p[2])
    q4 = m[4] - 0.5 * (m[0] + m[8])
    after = jnp.where(is_last, m[8], m16 + 0.21875 * o[15] + 0.25 * p[14])
    q12 = m[12] - 0.5 * (m[8] + after)
    before = jnp.where(is_first, q4, c0 - 0.03125 * x[0] - 0.125 * low[0] - 0.5 * m[0])
    y = dict(o)
    y.update(p)
    y[4] = q4
    y[12] = q12
    y[0] = m[0] + 0.25 * (before + q4)
    y[8] = m[8] + 0.25 * (q4 + q12)
    return [y[n] for n in range(SPAN)]


def edges_kernel(group, chosen, *refs):
    given = len(chosen) * group
    to_right, to_left = refs[given:]
    _, rows, width = to_right.shape

    def variant(place):
        span = span_of(group, chosen, refs[:given], place)

        def body(r, c):
            right, left = partial_levels([ref[k, r, c] for ref, k in span])
            for k in range(TLEVELS):
                to_right[k, r, c] = right[k]
                to_left[k, r, c] = left[k]

        each_tile(rows, width, body)

    each_member(group, variant)


def time_kernel(group, chosen, *refs):
    given = len(chosen) * group
    left, right = refs[given : given + 2]
    pieces = refs[given + 2 : given + 2 + group]
    power = refs[given + 2 + group]
    frames = SPAN // group
    _, rows, width = left.shape
    spot = lax.axis_index("frame") // group
    is_first = spot == 0
    is_last = spot == lax.axis_size("frame") // group - 1

    @pl.when(pl.program_id(0) == 0)
    def _():
        power[...] = jnp.zeros_like(power)

    def variant(place):
        span = span_of(group, chosen, refs[:given], place)

        def body(r, c):
            y = full_levels(
                [ref[k, r, c] for ref, k in span],
                [left[k, r, c] for k in range(TLEVELS)],
                [right[k, r, c] for k in range(TLEVELS)],
                is_first,
                is_last,
            )
            sums = [None] * (TLEVELS + 1)
            for n in range(SPAN):
                t = level_of(n % 2**TLEVELS, TLEVELS) - 1
                square = y[n] * y[n]
                sums[t] = square if sums[t] is None else sums[t] + square
                if n % frames in KEPT:
                    pieces[place ^ (n // frames)][KEPT.index(n % frames), r, c] = y[n]
            for t in range(TLEVELS + 1):
                power[t, :, c] = power[t, :, c] + sums[t]

        each_tile(rows, width, body)

    each_member(group, variant)


def block_of(rows):
    return min(MOST_ROWS, rows // 2)


def span_specs(group, chosen, first, rows, width):
    block = block_of(rows)
    skip = first // block
    return [
        pl.BlockSpec((len(frames), block, width), lambda i: (0, skip + i, 0))
        for frames in chosen
        for _ in range(group)
    ]


def time_cost(rows, width, frames):
    return pl.CostEstimate(
        flops=rows * width * 2000, bytes_accessed=rows * width * 4 * frames, transcendentals=0
    )


def edges(group, first, rows, chosen, given):
    width = given[0].shape[2]
    spec = pl.BlockSpec((TLEVELS, block_of(rows), width), lambda i: (0, i, 0))
    shape = jax.ShapeDtypeStruct((TLEVELS, rows, width), jnp.float32)
    return pl.pallas_call(
        functools.partial(edges_kernel, group, chosen),
        grid=(rows // block_of(rows),),
        in_specs=span_specs(group, chosen, first, rows, width),
        out_specs=[spec, spec],
        out_shape=[shape, shape],
        cost_estimate=time_cost(rows, width, SPAN + 6),
    )(*given)


def finish_time(group, first, rows, chosen, given, left, right):
    width = given[0].shape[2]
    kept = len(KEPT)
    halo = pl.BlockSpec((TLEVELS, block_of(rows), width), lambda i: (0, i, 0))
    outs = pl.pallas_call(
        functools.partial(time_kernel, group, chosen),
        grid=(rows // block_of(rows),),
        in_specs=span_specs(group, chosen, first, rows, width) + [halo, halo],
        out_specs=[pl.BlockSpec((kept, block_of(rows), width), lambda i: (0, i, 0))] * group
        + [pl.BlockSpec((TLEVELS + 1, SUB, width), lambda i: (0, 0, 0))],
        out_shape=[jax.ShapeDtypeStruct((kept, rows, width), jnp.float32)] * group
        + [jax.ShapeDtypeStruct((TLEVELS + 1, SUB, width), jnp.float32)],
        cost_estimate=time_cost(rows, width, 2 * SPAN + 6),
    )(*given, left, right)
    return outs[:group], outs[group]


def home_kernel(group, strip, fresh, *refs):
    given = 3 * group
    out, held, sems = refs[given if fresh else given + 1 :]
    me = member(group)
    starts = [start for start, _ in strip]
    step = pl.program_id(0)

    def copy(d, at):
        start = part_start(starts, strip, me ^ d, group) + at * MOST_ROWS
        return pltpu.make_async_copy(
            held.at[at, d],
            out.at[1, pl.ds(pl.multiple_of(start, SUB), MOST_ROWS)],
            sems.at[at, d],
        )

    for d in range(group):
        held[step, d] = refs[group + d][0] - 0.5 * (refs[d][0] + refs[2 * group + d][0])
        copy(d, step).start()

    @pl.when(step == held.shape[0] - 1)
    def _():
        for at in range(held.shape[0]):
            for d in range(group):
                copy(d, at).wait()


def home(group, strip, chosen, sent, shape, coeffs):
    width = shape[2]
    part = strip_rows(strip) // group
    given, specs = [], []
    for f in range(3):
        u = [f in frames for frames in chosen].index(True)
        k = chosen[u].index(f)
        given += sent[u]
        specs += [pl.BlockSpec((1, MOST_ROWS, width), lambda i, k=k: (k, i, 0))] * group
    fresh = coeffs is None
    if not fresh:
        given.append(coeffs)
        specs.append(pl.BlockSpec(memory_space=pl.ANY))
    return pl.pallas_call(
        functools.partial(home_kernel, group, strip, fresh),
        grid=(part // MOST_ROWS,),
        in_specs=specs,
        out_specs=pl.BlockSpec(memory_space=pl.ANY),
        out_shape=jax.ShapeDtypeStruct(shape, jnp.float32),
        input_output_aliases={} if fresh else {3 * group: 0},
        scratch_shapes=[
            pltpu.VMEM((part // MOST_ROWS, group, MOST_ROWS, width), jnp.float32),
            pltpu.SemaphoreType.DMA((part // MOST_ROWS, group)),
        ],
        cost_estimate=time_cost(part, width, 4 * group),
    )(*given)


def place_kernel(group, strip, first, *refs):
    pieces, _, out, held, ins, outs = refs[:group], *refs[group:]
    kept, rows, _ = pieces[0].shape
    me = member(group)
    starts = [start for start, _ in strip]
    arriving, leaving = [], []
    for d in range(group):
        start = pl.multiple_of(part_start(starts, strip, me ^ d, group) + first, SUB)
        for k, f in enumerate(KEPT):
            n = d * kept + k
            arriving.append(pltpu.make_async_copy(pieces[d].at[k], held.at[n], ins.at[n]))
            leaving.append(
                pltpu.make_async_copy(held.at[n], out.at[f, pl.ds(start, rows)], outs.at[n])
            )
    for copy in arriving:
        copy.start()
    for copy, after in zip(arriving, leaving):
        copy.wait()
        after.start()
    for copy in leaving:
        copy.wait()


def place(group, strip, first, pieces, coeffs):
    kept, rows, width = pieces[0].shape
    count = group * kept
    return pl.pallas_call(
        functools.partial(place_kernel, group, strip, first),
        in_specs=[pl.BlockSpec(memory_space=pl.ANY)] * (group + 1),
        out_specs=pl.BlockSpec(memory_space=pl.ANY),
        out_shape=jax.ShapeDtypeStruct(coeffs.shape, coeffs.dtype),
        input_output_aliases={group: 0},
        scratch_shapes=[
            pltpu.VMEM((count, rows, width), jnp.float32),
            pltpu.SemaphoreType.DMA((count,)),
            pltpu.SemaphoreType.DMA((count,)),
        ],
        cost_estimate=time_cost(rows, width, 2 * count),
    )(*pieces, coeffs)


def swap(blocks, group):
    devices = range(lax.axis_size("frame"))
    out = [blocks[0]]
    for d in range(1, group):
        out.append(lax.ppermute(blocks[d], "frame", [(i, i ^ d) for i in devices]))
    return out


def shifted(block, axis, distance):
    devices = range(lax.axis_size(axis))
    route = [(i - distance, i) for i in devices if i - distance in devices]
    return lax.ppermute(block, axis, route)


def doubled(total, axis, bit):
    devices = range(lax.axis_size(axis))
    return total + lax.ppermute(total, axis, [(i, i ^ bit) for i in devices])


def tree_sum(parts):
    while len(parts) > 1:
        parts = [parts[k] + parts[k + 1] for k in range(0, len(parts), 2)]
    return parts[0]


def total_of_all(totals, group):
    row_size, frame_size = lax.axis_size("row"), lax.axis_size("frame")
    if row_size & (row_size - 1) or frame_size & (frame_size - 1):
        return lax.psum(totals, ("frame", "row"))
    devices = range(frame_size)
    unit = group
    while unit < frame_size:
        count = min(4, frame_size // unit)
        parts = [totals]
        for k in range(1, count):
            parts.append(lax.ppermute(totals, "frame", [(i, i ^ (unit * k)) for i in devices]))
        totals = tree_sum(parts)
        unit *= count
    bit = 1
    while bit < row_size:
        totals = doubled(totals, "row", bit)
        bit *= 2
    return tree_sum(swap([totals] * group, group))


def shards(footage):
    frames, rows, width = footage.shape
    group = SPAN // frames
    strips = strips_of(rows)
    weights = jnp.asarray(np.stack([column_weights(2**level) for level in range(SLEVELS)]))
    top = shifted(footage[:, rows - HALO :], "row", 1)
    bottom = shifted(footage[:, :HALO], "row", -1)
    sent, arrived, chosen = [[], []], [[], []], [[], []]
    for u, (which, own) in enumerate(UNITS):
        pieces = space(u, footage, top, bottom, weights, strips, group)
        sent[which].append(pieces)
        chosen[which].append(own)
        arrived[which] += swap(pieces, group)
    coeffs = None
    for which, strip in enumerate(strips):
        coeffs = home(group, strip, chosen[which], sent[which], footage.shape, coeffs)
    power = None
    back = []
    turns = turns_of(strips, group)
    for which, first, count in turns:
        given, own = arrived[which], chosen[which]
        to_right, to_left = edges(group, first, count, own, given)
        left = shifted(to_right, "frame", group)
        right = shifted(to_left, "frame", -group)
        pieces, part_power = finish_time(group, first, count, own, given, left, right)
        back.append(swap(pieces, group))
        power = part_power if power is None else power + part_power
    period = 2**SLEVELS
    column_phase = np.arange(width) % period
    selector = jnp.asarray((column_phase[:, None] == np.arange(period)[None, :]).astype(np.float32))
    pattern = jnp.dot(
        power.reshape((TLEVELS + 1) * SUB, width), selector, precision=lax.Precision.HIGHEST
    ).reshape(TLEVELS + 1, SUB * period)
    totals = jnp.dot(
        pattern, jnp.asarray(space_table(SLEVELS), jnp.float32), precision=lax.Precision.HIGHEST
    )
    totals = total_of_all(totals, group)
    for t, (which, first, _) in enumerate(turns):
        coeffs = place(group, strips[which], first, back[t], coeffs)
    means = band_means(
        totals,
        frames * lax.axis_size("frame"),
        rows * lax.axis_size("row"),
        width,
        SLEVELS,
        TLEVELS,
    )
    return (coeffs, means)


def solution(mesh):
    return jax.shard_map(
        shards,
        mesh=mesh,
        in_specs=(P("frame", "row", None),),
        out_specs=(P("frame", "row", None), P()),
        check_vma=False,
    )
```
